32 devices in a mesh: dp: 4 (over x, y), tp: 8 (over z, core).
Axes of the slice: x: 2, y: 2, z: 4, core: 2. Of those that a mesh axis runs over, the one named last changes fastest.
Arguments:
- x: bfloat16 [8192, 7168], P(('dp', 'tp')), parts along dimension 0
- dy: bfloat16 [8192, 7168], P(('dp', 'tp')), parts along dimension 0
- gain: bfloat16 [7168], replicated
- wq: bfloat16 [7168, 7168], P(None, 'tp')
- wk: bfloat16 [7168, 7168], P(None, 'tp')
- wv: bfloat16 [7168, 7168], P(None, 'tp')
- wo: bfloat16 [7168, 7168], P('tp')
Outputs:
- output 1: bfloat16 [8192, 7168], P(('dp', 'tp')), parts along dimension 0
- output 2: float32 [4, 7168], P('dp'), parts along dimension 0
- output 3: bfloat16 [28672, 7168], P('dp', 'tp'), parts along dimension 0
- output 4: bfloat16 [28672, 7168], P('dp', 'tp'), parts along dimension 0
- output 5: bfloat16 [28672, 7168], P('dp', 'tp'), parts along dimension 0
- output 6: bfloat16 [28672, 7168], P(('dp', 'tp')), parts along dimension 0
There are 4 independent parts. The reference program is written for one: setup_inputs(seed, part) draws one part's arguments, and reference() takes and returns one part's arrays. A program takes and returns all parts, laid end to end along the dimension named above; an argument that names none is the same for every part.
All inputs are finite; a program needn't handle non-finite values.
Results may differ from the reference program's by a relative error of at most 0.018.
Values are sent between devices in bfloat16 or wider.
A program may use at most 2 GiB of HBM per device.

```python
import jax
import jax.numpy as jnp
from jax import lax

ROWS = 2048
D = 7168
HEADS = 56
KV_HEADS = 56
HEAD = 128
THETA = 10000


def setup_inputs(seed: int = 0, part: int = 0) -> dict:
    kx, ky, kn, kq, kk, kv, ko = jax.random.split(jax.random.key(seed), 7)

    def weights(key, rows, columns):
        return jax.random.normal(key, (rows, columns), jnp.float32) * rows**-0.5

    drawn = {
        "x": jax.random.normal(jax.random.fold_in(kx, part), (ROWS, D), jnp.float32),
        "dy": jax.random.normal(jax.random.fold_in(ky, part), (ROWS, D), jnp.float32) * ROWS**-0.5,
        "gain": 1 + 0.1 * jax.random.normal(kn, (D,), jnp.float32),
        "wq": 2 * weights(kq, D, HEADS * HEAD),
        "wk": 2 * weights(kk, D, KV_HEADS * HEAD),
        "wv": 4 * weights(kv, D, KV_HEADS * HEAD),
        "wo": weights(ko, HEADS * HEAD, D),
    }
    return {k: v.astype(jnp.bfloat16) for k, v in drawn.items()}


def normed(x, gain):
    wide = x.astype(jnp.float32)
    scale = lax.rsqrt(jnp.mean(wide * wide, -1, keepdims=True) + 1e-6)
    return (wide * scale * gain.astype(jnp.float32)).astype(jnp.bfloat16)


def turned(t, place, theta):
    half = t.shape[-1] // 2
    angle = place.astype(jnp.float32)[:, None] * theta ** (-jnp.arange(half, dtype=jnp.float32) / half)
    cos, sin = jnp.cos(angle)[:, None], jnp.sin(angle)[:, None]
    a, b = t[..., :half].astype(jnp.float32), t[..., half:].astype(jnp.float32)
    return jnp.concatenate([a * cos - b * sin, b * cos + a * sin], -1).astype(jnp.bfloat16)


def matmul(a, w):
    return jnp.dot(a, w, preferred_element_type=jnp.float32).astype(jnp.bfloat16)


def einsum(form, a, b):
    return jnp.einsum(form, a.astype(jnp.float32), b.astype(jnp.float32))


def attention(q, k, v):
    scores = einsum("tgsd,ugd->gstu", q, k) * q.shape[-1] ** -0.5
    token = jnp.arange(q.shape[0])
    scores = jnp.where(token[:, None] >= token, scores, -jnp.inf)
    weights = jax.nn.softmax(scores, -1).astype(jnp.bfloat16)
    return einsum("gstu,ugd->tgsd", weights, v).astype(jnp.bfloat16)


def forward(x, gain, wq, wk, wv, wo):
    rows = x.shape[0]
    a, place = normed(x, gain), jnp.arange(rows)
    k = turned(matmul(a, wk).reshape(rows, -1, HEAD), place, THETA)
    q = turned(matmul(a, wq).reshape(rows, -1, HEAD), place, THETA).reshape(rows, k.shape[1], -1, HEAD)
    v = matmul(a, wv).reshape(rows, -1, HEAD)
    seen = attention(q, k, v).reshape(rows, -1)
    return (x.astype(jnp.float32) + jnp.dot(seen, wo, preferred_element_type=jnp.float32)).astype(jnp.bfloat16)


def reference(x, dy, gain, wq, wk, wv, wo):
    _, back = jax.vjp(forward, x, gain.astype(jnp.float32), wq, wk, wv, wo)
    by_x, by_gain, *by_weights = back(dy)
    return (by_x, by_gain[None], *by_weights)
```

```python
import functools

import jax
import jax.numpy as jnp
from jax import lax
from jax.experimental import pallas as pl
from jax.experimental.pallas import tpu as pltpu
from jax.sharding import PartitionSpec as P

HEAD = 128
THETA = 10000
LOG2E = 1.4426950408889634
HIDDEN = -2e30
VMEM = 56 * 2**20
BLOCK = 512
F32, BF16 = jnp.float32, jnp.bfloat16


def _dot(a, b, ca, cb):
    return lax.dot_general(a, b, (((ca,), (cb,)), ((), ())), preferred_element_type=F32)


def _size(rows):
    return max(n for n in (BLOCK, 256, 128) if rows % n == 0)


def _shown(b):
    return lax.broadcasted_iota(jnp.int32, (b, b), 1) >= lax.broadcasted_iota(jnp.int32, (b, b), 0)


def _turn(t, cos, sin):
    wide = t.astype(F32)
    return (wide * cos + pltpu.roll(wide, HEAD // 2, 1) * sin).astype(BF16)


def _forward(q_in, k_in, v_ref, cos_ref, sin_ref, q_ref, k_ref, o_ref, lse_ref, *, scale):
    rows = q_in.shape[0]
    b = _size(rows)
    e = scale * LOG2E
    for i in range(rows // b):
        at = pl.ds(i * b, b)
        q_ref[at, :] = _turn(q_in[at, :], cos_ref[at, :], sin_ref[at, :])
        k_ref[at, :] = _turn(k_in[at, :], cos_ref[at, :], sin_ref[at, :])
    ones = jnp.ones((8, b), BF16)
    for i in range(rows // b):
        q = q_ref[pl.ds(i * b, b), :]
        scores = [_dot(k_ref[pl.ds(j * b, b), :], q, 1, 1) for j in range(i + 1)]
        scores[i] = jnp.where(_shown(b), scores[i], HIDDEN)
        top = functools.reduce(jnp.maximum, [s.max(axis=0, keepdims=True) for s in scores])
        mix = None
        for j in range(i + 1):
            p = jnp.exp2((scores[j] - top) * e).astype(BF16)
            values = jnp.concatenate([v_ref[pl.ds(j * b, b), :].T, ones], axis=0)
            part = _dot(values, p, 1, 0)
            mix = part if mix is None else mix + part
        total = mix[HEAD : HEAD + 1, :]
        o_ref[pl.ds(i * b, b), :] = (mix[:HEAD, :] * (1 / total)).T.astype(BF16)
        lse_ref[0, :, pl.ds(i * b, b)] = (top * scale + jnp.log(total)) * LOG2E


def _backward(q_ref, k_ref, v_ref, o_ref, do_ref, lse_ref, cos_ref, sin_ref, dq_ref, dk_ref, dv_ref, dq_s, *, scale):
    rows = q_ref.shape[0]
    b = _size(rows)
    n = rows // b
    e = scale * LOG2E
    deltas = [(do_ref[pl.ds(i * b, b), :].astype(F32) * o_ref[pl.ds(i * b, b), :].astype(F32)).T.sum(axis=0, keepdims=True) for i in range(n)]
    for j in range(n):
        here = pl.ds(j * b, b)
        k, v = k_ref[here, :], v_ref[here, :]
        scores = [_dot(k, q_ref[pl.ds(i * b, b), :], 1, 1) for i in range(j, n)]
        dps = [_dot(v, do_ref[pl.ds(i * b, b), :], 1, 1) for i in range(j, n)]
        dk = dv = None
        for i in range(j, n):
            at = pl.ds(i * b, b)
            p = jnp.exp2(scores[i - j] * e - lse_ref[0, :, at])
            if i == j:
                p = jnp.where(_shown(b), p, 0.0)
            ds = (p * (dps[i - j] - deltas[i])).astype(BF16)
            by_v, by_k = _dot(p.astype(BF16), do_ref[at, :], 1, 0), _dot(ds, q_ref[at, :], 1, 0)
            dv, dk = (by_v, by_k) if dv is None else (dv + by_v, dk + by_k)
            by_q = _dot(k.T, ds, 1, 0)
            if j == 0:
                dq_s[:, at] = by_q
            else:
                dq_s[:, at] += by_q
        dk_ref[here, :] = _turn((dk * scale).astype(BF16), cos_ref[here, :], -sin_ref[here, :])
        dv_ref[here, :] = dv.astype(BF16)
        dq = (dq_s[:, here] * scale).T.astype(BF16)
        dq_ref[here, :] = _turn(dq, cos_ref[here, :], -sin_ref[here, :])


def _attention_call(kernel, args, outs, scratch, rows, heads, products):
    def spec(shape):
        if len(shape) == 3:
            return pl.BlockSpec((1, 1, rows), lambda h: (h, 0, 0))
        return pl.BlockSpec((rows, HEAD), (lambda h: (0, h)) if shape[1] == heads * HEAD and heads > 1 else (lambda h: (0, 0)))

    return pl.pallas_call(
        functools.partial(kernel, scale=HEAD**-0.5),
        grid=(heads,),
        in_specs=[spec(a.shape) for a in args],
        out_specs=[spec(s.shape) for s in outs],
        out_shape=outs,
        scratch_shapes=scratch,
        compiler_params=pltpu.CompilerParams(dimension_semantics=("parallel",), vmem_limit_bytes=VMEM),
        cost_estimate=pl.CostEstimate(flops=products * heads * rows * rows * HEAD * 2, transcendentals=heads * rows * rows,
                                      bytes_accessed=2 * rows * heads * HEAD * (len(args) + len(outs))),
    )(*args)


def _by_states(dq_ref, dk_ref, dv_ref, wq_ref, wk_ref, wv_ref, out_ref):
    total = _dot(dq_ref[...], wq_ref[...], 1, 1) + _dot(dk_ref[...], wk_ref[...], 1, 1) + _dot(dv_ref[...], wv_ref[...], 1, 1)
    out_ref[...] = total.astype(BF16)


def by_states(grads, weights, start, columns, tile=256):
    rows, inner = grads[0].shape
    return pl.pallas_call(
        _by_states,
        grid=(columns // tile,),
        in_specs=[pl.BlockSpec((rows, inner), lambda n: (0, 0))] * 3 + [pl.BlockSpec((tile, inner), lambda n: (n + start // tile, 0))] * 3,
        out_specs=pl.BlockSpec((rows, tile), lambda n: (0, n)),
        out_shape=jax.ShapeDtypeStruct((rows, columns), BF16),
        compiler_params=pltpu.CompilerParams(dimension_semantics=("parallel",), vmem_limit_bytes=VMEM),
        cost_estimate=pl.CostEstimate(flops=6 * rows * inner * columns, transcendentals=0,
                                      bytes_accessed=2 * (3 * rows * inner + 3 * inner * columns + rows * columns)),
    )(*grads, *weights)


def solution(mesh):
    ranks = mesh.shape["tp"]

    def group_sum(t):
        flips = (1, 2, 6) if ranks == 8 else ()
        if not flips:
            return lax.psum(t, "tp")
        for flip in flips:
            t = t + lax.ppermute(t, "tp", [(i, i ^ flip) for i in range(ranks)])
        return t

    def step(x, dy, gain, wq, wk, wv, wo):
        width = x.shape[1]
        head_columns = wq.shape[1]
        heads = head_columns // HEAD
        wide, gain = x.astype(F32), gain.astype(F32)

        def gathered(t):
            return lax.all_gather(t, "tp", axis=0, tiled=True)

        cut = width * 11 // 14
        scale = lax.rsqrt(jnp.mean(wide * wide, -1, keepdims=True) + 1e-6)
        some = gathered((wide * scale * gain).astype(BF16))
        rows = some.shape[0]
        first, last, some = lax.optimization_barrier((dy[:, :cut], dy[:, cut:], some))
        dy1, dy2 = gathered(first), gathered(last)

        half = HEAD // 2
        angle = jnp.arange(rows).astype(F32)[:, None] * THETA ** (-jnp.arange(half, dtype=F32) / half)
        cos, sin = jnp.cos(angle), jnp.sin(angle)
        cos, sin = jnp.concatenate([cos, cos], 1), jnp.concatenate([-sin, sin], 1)

        some, cos, sin = lax.optimization_barrier((some, cos, sin))
        q, k, v = (jnp.dot(some, w, preferred_element_type=F32).astype(BF16) for w in (wq, wk, wv))
        flat = jax.ShapeDtypeStruct((rows, head_columns), BF16)
        stats = jax.ShapeDtypeStruct((heads, 1, rows), F32)
        q, k, seen, lse = _attention_call(_forward, (q, k, v, cos, sin), (flat, flat, flat, stats), [], rows, heads, 1)

        seen, lse, dy1 = lax.optimization_barrier((seen, lse, dy1))

        d_seen = _dot(dy1, wo[:, :cut], 1, 1)
        by_wo1 = _dot(seen, dy1, 0, 0).astype(BF16)
        d_seen, by_wo1, dy2 = lax.optimization_barrier((d_seen, by_wo1, dy2))
        d_seen = (d_seen + _dot(dy2, wo[:, cut:], 1, 1)).astype(BF16)

        grads = _attention_call(_backward, (q, k, v, seen, d_seen, lse, cos, sin), (flat, flat, flat),
                                [pltpu.VMEM((HEAD, rows), F32)], rows, heads, 3)

        edges = (0, width // 7, width // 2, width)
        sums = []
        for p, q in zip(edges, edges[1:]):
            term = by_states(grads, (wq, wk, wv), p, q - p)
            grads, term = lax.optimization_barrier((grads, term))
            sums.append(lax.psum_scatter(term, "tp", scatter_dimension=0, tiled=True))

        by_weights = [_dot(some, g, 0, 0).astype(BF16) for g in grads]
        seen, _ = lax.optimization_barrier((seen, term))
        by_wo = jnp.concatenate([by_wo1, _dot(seen, dy2, 0, 0).astype(BF16)], axis=1)

        by_gain, along, sets = [], 0, []
        for total, at, end in zip(sums, edges, edges[1:]):
            g, w = total.astype(F32), wide[:, at:end]
            by_gain.append((g * (w * scale)).sum(0, keepdims=True))
            u = g * gain[None, at:end]
            along = along + (u * w).sum(1, keepdims=True)
            sets.append((u, w, dy[:, at:end].astype(F32)))
        back = along * scale * scale * scale / width
        by_x = jnp.concatenate([(d + (u * scale - w * back)).astype(BF16) for u, w, d in sets], axis=1)
        return (by_x, group_sum(jnp.concatenate(by_gain, 1)), *by_weights, by_wo)

    tokens, columns = P(("dp", "tp"), None), P(None, "tp")
    return jax.shard_map(
        step,
        mesh=mesh,
        in_specs=(tokens, tokens, P(None), columns, columns, columns, P("tp", None)),
        out_specs=(tokens, P("dp", None), P("dp", "tp"), P("dp", "tp"), P("dp", "tp"), P(("dp", "tp"), None)),
        check_vma=False,
    )
```
